32 devices in a mesh: frame: 8 (over z, x), row: 4 (over y, core).
Axes of the slice: x: 2, y: 2, z: 4, core: 2. Of those that a mesh axis runs over, the one named last changes fastest.
Arguments:
- clip: bfloat16 [16, 16, 256, 128], P('frame', 'row'), may hold values from -6 to 6
- first_kernel: bfloat16 [3, 3, 3, 128, 128], replicated, may hold values from -0.109375 to 0.109375
- second_kernel: bfloat16 [3, 3, 3, 128, 128], replicated, may hold values from -0.109375 to 0.109375
- cotangent: bfloat16 [16, 16, 256, 128], P('frame', 'row'), may hold values from -6 to 6
Outputs:
- critic_map: bfloat16 [16, 16, 256, 128], P('frame', 'row')
- clip_grad: bfloat16 [16, 16, 256, 128], P('frame', 'row')
- first_grad: float32 [3, 3, 3, 128, 128], replicated
- second_grad: float32 [3, 3, 3, 128, 128], replicated
The draws below stay inside these ranges and needn't reach their ends.
All inputs are finite; a program needn't handle non-finite values.
Results may differ from the reference program's by a relative error of at most 0.012.
Values may be sent and summed in bfloat16 or wider, within the bound.
No kernel may reach another device: no remote copies, remote signals or barrier semaphores. Data moves between devices by JAX's collectives and lax.ppermute only.
A program may use at most 64 MiB of HBM per device.

```python
import jax
import jax.numpy as jnp
from jax import lax

CH = 128
WIDTH = 256
FRAMES = 16
ROWS = 16


def level_of(stream_key, extent, shards, low, high):
    loudness = 1.0
    for position, parts in shards:
        draws = jax.random.uniform(jax.random.fold_in(jax.random.fold_in(stream_key, 6), position), (parts,), jnp.float32, low / len(shards), high / len(shards))
        loudness = loudness * jnp.repeat(jnp.exp(draws), extent[position] // parts).reshape((-1,) + (1,) * (len(extent) - 1 - position))
    return loudness


def centred(rng, extent, scale, most, cuts=(), held_as=jnp.bfloat16):
    gain = level_of(rng, extent, cuts, -0.22, 0.18) if cuts else 1.0
    values = jax.random.normal(rng, extent, jnp.float32) * scale * gain
    return jnp.minimum(jnp.maximum(values, -most), most).astype(held_as)


def setup_inputs(seed: int = 0) -> dict:
    key_list = jax.random.split(jax.random.key(seed), 5)
    clip = centred(key_list[0], (FRAMES, ROWS, WIDTH, CH), 1.0, 6.0, ((0, 8), (1, 4)))
    first_kernel = centred(key_list[1], (3, 3, 3, CH, CH), (27 * CH) ** -0.5, 0.109375)
    second_kernel = centred(key_list[2], (3, 3, 3, CH, CH), (27 * CH) ** -0.5, 0.109375)
    cotangent = centred(key_list[3], (FRAMES, ROWS, WIDTH, CH), 1.0, 6.0, ((0, 8), (1, 4)))
    return dict(clip=clip, first_kernel=first_kernel, second_kernel=second_kernel, cotangent=cotangent)


def correlate(padded, kernel):
    result = lax.conv_general_dilated(padded[None], kernel, (1, 1, 1), ((0, 0), (0, 0), (1, 1)), dimension_numbers=('NDHWC', 'DHWIO', 'NDHWC'), preferred_element_type=jnp.float32)
    return result[0]

def silu_slope(value):
    sigma = jax.nn.sigmoid(value)
    return sigma * (1.0 + value * (1.0 - sigma))

def flipped_kernel(kernel):
    return jnp.transpose(kernel[::-1, ::-1, ::-1], (0, 1, 2, 4, 3))

def weight_grad(padded, delta):
    frame_count, row_count, columns, channels = delta.shape
    widened = jnp.pad(padded, ((0, 0), (0, 0), (1, 1), (0, 0)))
    flat_delta = delta.reshape(-1, channels)
    blocks = []
    for frame_off in range(3):
        for row_off in range(3):
            for col_off in range(3):
                window_slab = widened[frame_off:frame_off + frame_count, row_off:row_off + row_count, col_off:col_off + columns]
                blocks.append(lax.dot_general(window_slab.reshape(-1, channels), flat_delta, (((0,), (0,)), ((), ())), preferred_element_type=jnp.float32))
    return jnp.stack(blocks).reshape(3, 3, 3, channels, channels)

def reference(clip, first_kernel, second_kernel, cotangent):
    grad_scale = 1.0 / float(FRAMES * ROWS * WIDTH) ** 0.5
    clip_pad = jnp.pad(clip, ((2, 0), (1, 1), (0, 0), (0, 0)))
    first_pre = correlate(clip_pad, first_kernel)
    first_act = jax.nn.silu(first_pre).astype(jnp.bfloat16)
    act_pad = jnp.pad(first_act, ((2, 0), (1, 1), (0, 0), (0, 0)))
    second_pre = correlate(act_pad, second_kernel)
    critic_map = jax.nn.silu(second_pre).astype(jnp.bfloat16)
    second_delta = (cotangent.astype(jnp.float32) * silu_slope(second_pre)).astype(jnp.bfloat16)
    second_grad = weight_grad(act_pad, second_delta) * grad_scale
    first_back = correlate(jnp.pad(second_delta, ((0, 2), (1, 1), (0, 0), (0, 0))), flipped_kernel(second_kernel))
    first_delta = (first_back * silu_slope(first_pre)).astype(jnp.bfloat16)
    first_grad = weight_grad(clip_pad, first_delta) * grad_scale
    clip_grad = correlate(jnp.pad(first_delta, ((0, 2), (1, 1), (0, 0), (0, 0))), flipped_kernel(first_kernel)).astype(jnp.bfloat16)
    return (critic_map, clip_grad, first_grad, second_grad)
```

```python
import jax
import jax.numpy as jnp
from jax import lax
from jax.experimental import pallas as pl
from jax.experimental.pallas import tpu as pltpu
from jax.sharding import PartitionSpec as P

TAPS = 3
BF = jnp.bfloat16
F32 = jnp.float32


def shifted(rows):
    n, width, ch = rows.shape
    flat = rows.reshape(n * width, ch).astype(F32)
    col = lax.broadcasted_iota(jnp.int32, (n, width, ch), 1)
    before = pltpu.roll(flat, 1, 0).reshape(n, width, ch)
    after = pltpu.roll(flat, n * width - 1, 0).reshape(n, width, ch)
    before = jnp.where(col == 0, 0.0, before).astype(BF)
    after = jnp.where(col == width - 1, 0.0, after).astype(BF)
    return before, rows, after


def fill(win, own, other, own_first):
    ch = own[0].shape[-1]
    frames, height = own[0].shape[:2]
    first = (0, frames) if own_first else (2, 0)
    for start, (body, top, bottom), count in ((first[0], own, frames), (first[1], other, 2)):
        for f in range(count):
            for ref, row, size in ((top, 0, 1), (body, 1, height), (bottom, height + 1, 1)):
                for c, part in enumerate(shifted(ref[f])):
                    win[start + f, row : row + size, :, c * ch : (c + 1) * ch] = part


def window_product(win, weights, frames, height):
    width = win.shape[2]
    taps = [(f, b) for f in range(frames + 2) for b in range(TAPS)]
    acc = None
    for n in range(0, len(taps), 2):
        group = taps[n : n + 2]
        lhs = [win[f, b : b + height].reshape(height * width, win.shape[3]) for f, b in group]
        rhs = weights[n : n + len(group)].reshape(-1, weights.shape[2])
        lhs = jnp.concatenate(lhs, axis=1) if len(lhs) > 1 else lhs[0]
        part = jnp.dot(lhs, rhs, preferred_element_type=F32)
        acc = part if acc is None else acc + part
    return acc


def call(body, outs, scratch, *args):
    return pl.pallas_call(
        body,
        out_shape=outs,
        scratch_shapes=scratch,
        compiler_params=pltpu.CompilerParams(vmem_limit_bytes=56 << 20),
    )(*args)


def prepare(first_kernel, second_kernel, frames):
    ch = first_kernel.shape[-1]
    shape = ((frames + 2) * TAPS, TAPS * ch, frames * ch)

    def body(k1, k2, *outs):
        for kernel, ahead, back in ((k1, outs[0], outs[1]), (k2, outs[2], outs[3])):
            ahead[...] = jnp.zeros(shape, BF)
            back[...] = jnp.zeros(shape, BF)
            for a in range(TAPS):
                for b in range(TAPS):
                    for c in range(TAPS):
                        w = kernel[a, b, c]
                        wt = w.astype(F32).T.astype(BF)
                        a2, b2, c2 = TAPS - 1 - a, TAPS - 1 - b, TAPS - 1 - c
                        for t in range(frames):
                            o = slice(t * ch, (t + 1) * ch)
                            ahead[(t + a) * TAPS + b, c * ch : (c + 1) * ch, o] = w
                            back[(t + a2) * TAPS + b2, c2 * ch : (c2 + 1) * ch, o] = wt

    return call(body, [jax.ShapeDtypeStruct(shape, BF)] * 4, [], first_kernel, second_kernel)


def window_scratch(shape):
    frames, height, width, ch = shape
    return pltpu.VMEM((frames + 2, height + 2, width, TAPS * ch), BF)


def sigmoid(z):
    return 1.0 / (1.0 + jnp.exp(-z))


def first_layer(own, other, weights):
    shape = own[0].shape
    frames, height, width, ch = shape

    def body(x, xt, xb, y, yt, yb, w, act, slope, win):
        fill(win, (x, xt, xb), (y, yt, yb), False)
        acc = window_product(win, w, frames, height)
        s = sigmoid(acc)
        a = (acc * s).astype(BF)
        d = s * (1.0 + acc * (1.0 - s))
        for t in range(frames):
            o = slice(t * ch, (t + 1) * ch)
            act[t] = a[:, o].reshape(height, width, ch)
            slope[t] = d[:, o].reshape(height, width, ch)

    outs = [jax.ShapeDtypeStruct(shape, BF), jax.ShapeDtypeStruct(shape, F32)]
    return call(body, outs, [window_scratch(shape)], *own, *other, weights)


def second_layer(own, other, weights, cotangent):
    shape = own[0].shape
    frames, height, width, ch = shape

    def body(x, xt, xb, y, yt, yb, w, cot, out, delta, win):
        fill(win, (x, xt, xb), (y, yt, yb), False)
        acc = window_product(win, w, frames, height)
        s = sigmoid(acc)
        a = (acc * s).astype(BF)
        d = s * (1.0 + acc * (1.0 - s))
        for t in range(frames):
            o = slice(t * ch, (t + 1) * ch)
            out[t] = a[:, o].reshape(height, width, ch)
            delta[t] = (cot[t].astype(F32) * d[:, o].reshape(height, width, ch)).astype(BF)

    outs = [jax.ShapeDtypeStruct(shape, BF)] * 2
    return call(body, outs, [window_scratch(shape)], *own, *other, weights, cotangent)


def input_grad(own, other, weights, slope=None):
    shape = own[0].shape
    frames, height, width, ch = shape

    def body(x, xt, xb, y, yt, yb, w, *rest):
        out, win = rest[-2:]
        fill(win, (x, xt, xb), (y, yt, yb), True)
        acc = window_product(win, w, frames, height)
        for t in range(frames):
            part = acc[:, t * ch : (t + 1) * ch].reshape(height, width, ch)
            if slope is not None:
                part = part * rest[0][t]
            out[t] = part.astype(BF)

    extra = () if slope is None else (slope,)
    return call(body, jax.ShapeDtypeStruct(shape, BF), [window_scratch(shape)], *own, *other, weights, *extra)


def weight_grad(own, other, delta, scale, chunks, padded):
    shape = own[0].shape
    frames, height, width, ch = shape
    per_chunk = TAPS**3 * ch // chunks

    def body(x, xt, xb, y, yt, yb, d, out, win, sums):
        fill(win, (x, xt, xb), (y, yt, yb), False)
        if padded > per_chunk:
            out[:, per_chunk:] = jnp.zeros((chunks, padded - per_chunk, ch), BF)
        wide = jnp.concatenate([d[t].reshape(height * width, ch) for t in range(frames)], axis=1)
        turned = wide.T
        for f in range(frames + 2):
            rhs = [win[f, b : b + height].reshape(height * width, TAPS * ch) for b in range(TAPS)]
            part = jnp.dot(turned, jnp.concatenate(rhs, axis=1), preferred_element_type=F32)
            for t in range(frames):
                a = f - t
                if 0 <= a < TAPS:
                    mine = part[t * ch : (t + 1) * ch]
                    sums[a] = mine if t == 0 else sums[a] + mine
        for n in range(TAPS**3):
            a, bc = divmod(n, TAPS * TAPS)
            block = (sums[a, :, bc * ch : (bc + 1) * ch].T * scale).astype(BF)
            row = n * ch
            while row < (n + 1) * ch:
                chunk, at = divmod(row, per_chunk)
                size = min((n + 1) * ch - row, per_chunk - at)
                out[chunk, at : at + size] = block[row - n * ch : row - n * ch + size]
                row += size

    scratch = [window_scratch(shape), pltpu.VMEM((TAPS, ch, TAPS * TAPS * ch), F32)]
    out = jax.ShapeDtypeStruct((chunks, padded, ch), BF)
    return call(body, out, scratch, *own, *other, delta)


def exchanged(value, step):
    frames, rows = lax.axis_size("frame"), lax.axis_size("row")
    near = value[-2:] if step > 0 else value[:2]
    top, bottom = value[:, :1], value[:, -1:]
    near_top, near_bottom = near[:, :1], near[:, -1:]
    along = [(i, i + step) for i in range(frames) if 0 <= i + step < frames]
    both = ("frame", "row")
    other = lax.ppermute(near, "frame", along)
    down = [(i * rows + j, k * rows + j + 1) for i, k in along for j in range(rows - 1)]
    up = [(i * rows + j + 1, k * rows + j) for i, k in along for j in range(rows - 1)]
    other_top = lax.ppermute(near_bottom, both, down)
    other_bottom = lax.ppermute(near_top, both, up)
    own_top = lax.ppermute(bottom, "row", [(j, j + 1) for j in range(rows - 1)])
    own_bottom = lax.ppermute(top, "row", [(j + 1, j) for j in range(rows - 1)])
    return (value, own_top, own_bottom), (other, other_top, other_bottom)


def bits(axis):
    size = lax.axis_size(axis)
    return [(axis, n) for n in range(size.bit_length() - 1)]


def reduced(value):
    ch = value.shape[-1]
    order = bits("row") + bits("frame")
    part = value.reshape(-1, ch)
    for axis, n in order:
        mine = (lax.axis_index(axis) >> n) & 1
        halves = part.reshape(2, -1, ch)
        sent = lax.dynamic_index_in_dim(halves, 1 - mine, 0, False).astype(BF)
        kept = lax.dynamic_index_in_dim(halves, mine, 0, False).astype(F32)
        pairs = [(i, i ^ (1 << n)) for i in range(lax.axis_size(axis))]
        part = kept + lax.ppermute(sent, axis, pairs).astype(F32)
    part = part.astype(BF)
    for axis, n in reversed(order):
        mine = (lax.axis_index(axis) >> n) & 1
        pairs = [(i, i ^ (1 << n)) for i in range(lax.axis_size(axis))]
        got = lax.ppermute(part, axis, pairs)
        part = jnp.where(mine == 0, jnp.concatenate([part, got]), jnp.concatenate([got, part]))
    return part.reshape(value.shape)


def on_device(clip, first_kernel, second_kernel, cotangent):
    frames, height, width, ch = clip.shape
    n_frame, n_row = lax.axis_size("frame"), lax.axis_size("row")
    grad_scale = 1.0 / float(frames * n_frame * height * n_row * width) ** 0.5
    rows = TAPS**3 * ch // n_row
    unit = 16 * n_frame
    padded = -(-rows // unit) * unit

    def finish(grad):
        return reduced(grad)[:, :rows].astype(F32).reshape(TAPS, TAPS, TAPS, ch, ch)

    clip_near = exchanged(clip, 1)
    first_ahead, first_back, second_ahead, second_back = prepare(first_kernel, second_kernel, frames)
    act, slope = first_layer(*clip_near, first_ahead)
    act_near = exchanged(act, 1)
    critic_map, second_delta = second_layer(*act_near, second_ahead, cotangent)
    second_near = exchanged(second_delta, -1)
    second_grad = finish(weight_grad(*act_near, second_delta, grad_scale, n_row, padded))
    first_delta = input_grad(*second_near, second_back, slope)
    first_near = exchanged(first_delta, -1)
    first_grad = finish(weight_grad(*clip_near, first_delta, grad_scale, n_row, padded))
    clip_grad = input_grad(*first_near, first_back)
    return critic_map, clip_grad, first_grad, second_grad


def solution(mesh):
    placed = (P("frame", "row", None, None), P(), P(), P("frame", "row", None, None))
    return jax.shard_map(
        on_device,
        mesh=mesh,
        in_specs=placed,
        out_specs=(P("frame", "row", None, None), P("frame", "row", None, None), P(), P()),
        check_vma=False,
    )
```

```python
import jax
import jax.numpy as jnp
from jax import lax
from jax.experimental import pallas as pl
from jax.experimental.pallas import tpu as pltpu
from jax.sharding import PartitionSpec as P

TAPS = 3
BF = jnp.bfloat16
F32 = jnp.float32


def shifted(rows):
    n, width, ch = rows.shape
    flat = rows.reshape(n * width, ch).astype(F32)
    col = lax.broadcasted_iota(jnp.int32, (n, width, ch), 1)
    before = pltpu.roll(flat, 1, 0).reshape(n, width, ch)
    after = pltpu.roll(flat, n * width - 1, 0).reshape(n, width, ch)
    before = jnp.where(col == 0, 0.0, before).astype(BF)
    after = jnp.where(col == width - 1, 0.0, after).astype(BF)
    return before, rows, after


def fill(win, own, other, own_first):
    ch = own[0].shape[-1]
    frames, height = own[0].shape[:2]
    first = (0, frames) if own_first else (2, 0)
    for start, (body, top, bottom), count in ((first[0], own, frames), (first[1], other, 2)):
        for f in range(count):
            for ref, row, size in ((top, 0, 1), (body, 1, height), (bottom, height + 1, 1)):
                for c, part in enumerate(shifted(ref[f])):
                    win[start + f, row : row + size, :, c * ch : (c + 1) * ch] = part


def window_product(win, weights, frames, height):
    width = win.shape[2]
    taps = [(f, b) for f in range(frames + 2) for b in range(TAPS)]
    acc = None
    for n in range(0, len(taps), 2):
        group = taps[n : n + 2]
        lhs = [win[f, b : b + height].reshape(height * width, win.shape[3]) for f, b in group]
        rhs = weights[n : n + len(group)].reshape(-1, weights.shape[2])
        lhs = jnp.concatenate(lhs, axis=1) if len(lhs) > 1 else lhs[0]
        part = jnp.dot(lhs, rhs, preferred_element_type=F32)
        acc = part if acc is None else acc + part
    return acc


def call(body, outs, scratch, *args):
    return pl.pallas_call(
        body,
        out_shape=outs,
        scratch_shapes=scratch,
        compiler_params=pltpu.CompilerParams(vmem_limit_bytes=28 << 20),
    )(*args)


def prepare(first_kernel, second_kernel, frames):
    ch = first_kernel.shape[-1]
    shape = ((frames + 2) * TAPS, TAPS * ch, frames * ch)

    def body(k1, k2, *outs):
        for kernel, ahead, back in ((k1, outs[0], outs[1]), (k2, outs[2], outs[3])):
            ahead[...] = jnp.zeros(shape, BF)
            back[...] = jnp.zeros(shape, BF)
            for a in range(TAPS):
                for b in range(TAPS):
                    for c in range(TAPS):
                        w = kernel[a, b, c]
                        wt = w.astype(F32).T.astype(BF)
                        a2, b2, c2 = TAPS - 1 - a, TAPS - 1 - b, TAPS - 1 - c
                        for t in range(frames):
                            o = slice(t * ch, (t + 1) * ch)
                            ahead[(t + a) * TAPS + b, c * ch : (c + 1) * ch, o] = w
                            back[(t + a2) * TAPS + b2, c2 * ch : (c2 + 1) * ch, o] = wt

    return call(body, [jax.ShapeDtypeStruct(shape, BF)] * 4, [], first_kernel, second_kernel)


def window_scratch(shape):
    frames, height, width, ch = shape
    return pltpu.VMEM((frames + 2, height + 2, width, TAPS * ch), BF)


def sigmoid(z):
    return 1.0 / (1.0 + jnp.exp(-z))


def first_layer(own, other, weights):
    shape = own[0].shape
    frames, height, width, ch = shape

    def body(x, xt, xb, y, yt, yb, w, act, slope, win):
        fill(win, (x, xt, xb), (y, yt, yb), False)
        acc = window_product(win, w, frames, height)
        s = sigmoid(acc)
        a = (acc * s).astype(BF)
        d = s * (1.0 + acc * (1.0 - s))
        for t in range(frames):
            o = slice(t * ch, (t + 1) * ch)
            act[t] = a[:, o].reshape(height, width, ch)
            slope[t] = d[:, o].reshape(height, width, ch)

    outs = [jax.ShapeDtypeStruct(shape, BF), jax.ShapeDtypeStruct(shape, F32)]
    return call(body, outs, [window_scratch(shape)], *own, *other, weights)


def second_layer(own, other, weights, cotangent):
    shape = own[0].shape
    frames, height, width, ch = shape

    def body(x, xt, xb, y, yt, yb, w, cot, out, delta, win):
        fill(win, (x, xt, xb), (y, yt, yb), False)
        acc = window_product(win, w, frames, height)
        s = sigmoid(acc)
        a = (acc * s).astype(BF)
        d = s * (1.0 + acc * (1.0 - s))
        for t in range(frames):
            o = slice(t * ch, (t + 1) * ch)
            out[t] = a[:, o].reshape(height, width, ch)
            delta[t] = (cot[t].astype(F32) * d[:, o].reshape(height, width, ch)).astype(BF)

    outs = [jax.ShapeDtypeStruct(shape, BF)] * 2
    return call(body, outs, [window_scratch(shape)], *own, *other, weights, cotangent)


def input_grad(own, other, weights, slope=None):
    shape = own[0].shape
    frames, height, width, ch = shape

    def body(x, xt, xb, y, yt, yb, w, *rest):
        out, win = rest[-2:]
        fill(win, (x, xt, xb), (y, yt, yb), True)
        acc = window_product(win, w, frames, height)
        for t in range(frames):
            part = acc[:, t * ch : (t + 1) * ch].reshape(height, width, ch)
            if slope is not None:
                part = part * rest[0][t]
            out[t] = part.astype(BF)

    extra = () if slope is None else (slope,)
    return call(body, jax.ShapeDtypeStruct(shape, BF), [window_scratch(shape)], *own, *other, weights, *extra)


def weight_grad(own, other, delta, scale, chunks, padded):
    shape = own[0].shape
    frames, height, width, ch = shape
    per_chunk = TAPS**3 * ch // chunks

    def body(x, xt, xb, y, yt, yb, d, out, win, sums):
        fill(win, (x, xt, xb), (y, yt, yb), False)
        if padded > per_chunk:
            out[:, per_chunk:] = jnp.zeros((chunks, padded - per_chunk, ch), BF)
        wide = jnp.concatenate([d[t].reshape(height * width, ch) for t in range(frames)], axis=1)
        turned = wide.T
        for f in range(frames + 2):
            rhs = [win[f, b : b + height].reshape(height * width, TAPS * ch) for b in range(TAPS)]
            part = jnp.dot(turned, jnp.concatenate(rhs, axis=1), preferred_element_type=F32)
            for t in range(frames):
                a = f - t
                if 0 <= a < TAPS:
                    mine = part[t * ch : (t + 1) * ch]
                    sums[a] = mine if t == 0 else sums[a] + mine
        for n in range(TAPS**3):
            a, bc = divmod(n, TAPS * TAPS)
            block = (sums[a, :, bc * ch : (bc + 1) * ch].T * scale).astype(BF)
            row = n * ch
            while row < (n + 1) * ch:
                chunk, at = divmod(row, per_chunk)
                size = min((n + 1) * ch - row, per_chunk - at)
                out[chunk, at : at + size] = block[row - n * ch : row - n * ch + size]
                row += size

    scratch = [window_scratch(shape), pltpu.VMEM((TAPS, ch, TAPS * TAPS * ch), F32)]
    out = jax.ShapeDtypeStruct((chunks, padded, ch), BF)
    return call(body, out, scratch, *own, *other, delta)


def exchanged(value, step):
    frames, rows = lax.axis_size("frame"), lax.axis_size("row")
    near = value[-2:] if step > 0 else value[:2]
    top, bottom = value[:, :1], value[:, -1:]
    near_top, near_bottom = near[:, :1], near[:, -1:]
    along = [(i, i + step) for i in range(frames) if 0 <= i + step < frames]
    both = ("frame", "row")
    other = lax.ppermute(near, "frame", along)
    down = [(i * rows + j, k * rows + j + 1) for i, k in along for j in range(rows - 1)]
    up = [(i * rows + j + 1, k * rows + j) for i, k in along for j in range(rows - 1)]
    other_top = lax.ppermute(near_bottom, both, down)
    other_bottom = lax.ppermute(near_top, both, up)
    own_top = lax.ppermute(bottom, "row", [(j, j + 1) for j in range(rows - 1)])
    own_bottom = lax.ppermute(top, "row", [(j + 1, j) for j in range(rows - 1)])
    return (value, own_top, own_bottom), (other, other_top, other_bottom)


def bits(axis):
    size = lax.axis_size(axis)
    return [(axis, n) for n in range(size.bit_length() - 1)]


def reduced(value):
    ch = value.shape[-1]
    order = bits("row") + bits("frame")
    part = value.reshape(-1, ch)
    for axis, n in order:
        mine = (lax.axis_index(axis) >> n) & 1
        halves = part.reshape(2, -1, ch)
        sent = lax.dynamic_index_in_dim(halves, 1 - mine, 0, False).astype(BF)
        kept = lax.dynamic_index_in_dim(halves, mine, 0, False).astype(F32)
        pairs = [(i, i ^ (1 << n)) for i in range(lax.axis_size(axis))]
        part = kept + lax.ppermute(sent, axis, pairs).astype(F32)
    part = part.astype(BF)
    for axis, n in reversed(order):
        mine = (lax.axis_index(axis) >> n) & 1
        pairs = [(i, i ^ (1 << n)) for i in range(lax.axis_size(axis))]
        got = lax.ppermute(part, axis, pairs)
        part = jnp.where(mine == 0, jnp.concatenate([part, got]), jnp.concatenate([got, part]))
    return part.reshape(value.shape)


def on_device(clip, first_kernel, second_kernel, cotangent):
    frames, height, width, ch = clip.shape
    n_frame, n_row = lax.axis_size("frame"), lax.axis_size("row")
    grad_scale = 1.0 / float(frames * n_frame * height * n_row * width) ** 0.5
    rows = TAPS**3 * ch // n_row
    unit = 16 * n_frame
    padded = -(-rows // unit) * unit

    def finish(grad):
        return reduced(grad)[:, :rows].astype(F32).reshape(TAPS, TAPS, TAPS, ch, ch)

    clip_near = exchanged(clip, 1)
    first_ahead, first_back, second_ahead, second_back = prepare(first_kernel, second_kernel, frames)
    act, slope = first_layer(*clip_near, first_ahead)
    act_near = exchanged(act, 1)
    critic_map, second_delta = second_layer(*act_near, second_ahead, cotangent)
    second_near = exchanged(second_delta, -1)
    second_part = weight_grad(*act_near, second_delta, grad_scale, n_row, padded)
    second_grad = finish(second_part)
    first_delta = input_grad(*second_near, second_back, slope)
    first_near = exchanged(first_delta, -1)
    first_part = weight_grad(*clip_near, first_delta, grad_scale, n_row, padded)
    first_grad = finish(first_part)
    clip_grad = input_grad(*first_near, first_back)
    return critic_map, clip_grad, first_grad, second_grad


def solution(mesh):
    placed = (P("frame", "row", None, None), P(), P(), P("frame", "row", None, None))
    return jax.shard_map(
        on_device,
        mesh=mesh,
        in_specs=placed,
        out_specs=(P("frame", "row", None, None), P("frame", "row", None, None), P(), P()),
        check_vma=False,
    )
```
